32 devices in a mesh: pp: 4 (over x, core), tp: 2 (over y), dp: 4 (over z).
Axes of the slice: x: 2, y: 2, z: 4, core: 2. Of those that a mesh axis runs over, the one named last changes fastest.
Arguments:
- layer_input: bfloat16 [4, 4, 16, 4096], P('pp', 'dp', 'tp'), may hold values from -4 to 4
- gate_pre: bfloat16 [4, 4, 16, 14784], P('pp', 'dp', None, 'tp'), may hold values from -8 to 8
- up_pre: bfloat16 [4, 4, 16, 14784], P('pp', 'dp', None, 'tp'), may hold values from -6 to 6
- hidden_grad: bfloat16 [4, 4, 16, 14784], P('pp', 'dp', None, 'tp'), may hold values from -0.59765625 to 0.59765625
- gate_weight: bfloat16 [4, 4096, 14784], P('pp', 'dp', 'tp'), may hold values from -0.09375 to 0.09375
Outputs:
- passed_grad: bfloat16 [4, 4, 16, 4096], P('pp', 'dp', 'tp')
- gate_weight_grad: bfloat16 [4, 4096, 14784], P('pp', 'dp', 'tp')
The draws below stay inside these ranges and needn't reach their ends.
All inputs are finite; a program needn't handle non-finite values.
Results may differ from the reference program's by a relative error of at most 0.018.
Values may be sent and summed in bfloat16 or wider, within the bound.
A program may use at most 128 MiB of HBM per device.

```python
import jax
import jax.numpy as jnp
from jax import lax

D = 4096
FF = 14784
GROUP_TOKENS = 16
SECTIONS = 4
REPLICAS = 4
N_PP = 4
N_DP = 4


def spiked(drawn, stream_key, source, target, parts, factor):
    def block_of(dim):
        return (jnp.arange(drawn.shape[dim]) // (drawn.shape[dim] // parts)).reshape((-1,) + (1,) * (drawn.ndim - 1 - dim))

    first = jax.random.permutation(stream_key, parts)[block_of(target)]
    second = (block_of(target) + parts // 2) % parts
    return jnp.where((block_of(source) == first) | (block_of(source) == second), factor * drawn, drawn)


def levels(own_key, extent, pieces, smallest, high):
    loudness = 1.0
    for dim, parts in pieces:
        draws = jax.random.uniform(jax.random.fold_in(jax.random.fold_in(own_key, 6), dim), (parts,), jnp.float32, smallest / len(pieces), high / len(pieces))
        loudness = loudness * jnp.repeat(jnp.exp(draws), extent[dim] // parts).reshape((-1,) + (1,) * (len(extent) - 1 - dim))
    return loudness


def centred(stream_key, extent, width, bound, pieces=(), kind=jnp.bfloat16):
    values = jax.random.normal(stream_key, extent, jnp.float32) * width
    if len(pieces) > 0:
        values = levels(stream_key, extent, pieces, -0.22, 0.18) * values
    return jnp.clip(values, min=-bound, max=bound).astype(kind)


def heavy_noise(rng, shape, scale, limit, cuts, heavy, held_as=jnp.bfloat16):
    result = scale * jax.random.normal(rng, shape, jnp.float32)
    if cuts:
        result = result * levels(rng, shape, cuts, -0.22, 0.18)
    return jnp.clip(spiked(result, jax.random.fold_in(rng, 3), *heavy), -limit, limit).astype(held_as)


def setup_inputs(seed: int = 0) -> dict:
    keys = jax.random.split(jax.random.key(seed), 6)
    layer_input = heavy_noise(keys[0], (SECTIONS, REPLICAS, GROUP_TOKENS, D), 0.5, 4.0, ((0, 4), (1, 4), (2, 2)), (1, 3, 4, 2.0))
    gate_pre = centred(keys[1], (SECTIONS, REPLICAS, GROUP_TOKENS, FF), 1.5, 8.0, ((0, 4), (1, 4), (3, 2)))
    up_pre = centred(keys[2], (SECTIONS, REPLICAS, GROUP_TOKENS, FF), 1.0, 6.0, ((0, 4), (1, 4), (3, 2)))
    hidden_grad = centred(keys[3], (SECTIONS, REPLICAS, GROUP_TOKENS, FF), 0.1, 0.59765625, ((0, 4), (1, 4), (3, 2)))
    gate_weight = centred(keys[4], (SECTIONS, D, FF), D ** -0.5, 0.09375, ((0, 4), (1, 4), (2, 2)))
    return {"layer_input": layer_input, "gate_pre": gate_pre, "up_pre": up_pre, "hidden_grad": hidden_grad, "gate_weight": gate_weight}


def local_grad(gate_act, up_act, hidden):
    gate_val = gate_act.astype(jnp.float32)
    up_val = up_act.astype(jnp.float32)
    hidden_val = hidden.astype(jnp.float32)
    logistic = jax.nn.sigmoid(gate_val)
    return (hidden_val * up_val * logistic * (1.0 + gate_val * (1.0 - logistic))).astype(jnp.bfloat16)

def reference(layer_input, gate_pre, up_pre, hidden_grad, gate_weight):
    input_list = []
    gate_list = []
    for which_section in range(N_PP):
        gate_total = jnp.zeros((D, FF), jnp.float32)
        replica_grads = []
        for replica in range(N_DP):
            gate_grad = local_grad(gate_pre[which_section, replica], up_pre[which_section, replica], hidden_grad[which_section, replica])
            summed = jnp.dot(gate_grad, gate_weight[which_section].T, preferred_element_type=jnp.float32)
            replica_grads.append(summed.astype(jnp.bfloat16))
            tokens_in = layer_input[which_section, replica]
            gate_term = lax.optimization_barrier(jnp.dot(tokens_in.T, gate_grad, preferred_element_type=jnp.float32).astype(jnp.bfloat16))
            gate_total = gate_total + gate_term.astype(jnp.float32)
        input_list.append(jnp.stack(replica_grads))
        gate_list.append(gate_total.astype(jnp.bfloat16))
    zeros_last = jnp.zeros_like(input_list[0])
    passed_grad = jnp.stack(input_list[1:] + [zeros_last])
    return (passed_grad, jnp.stack(gate_list))
```

```python
import functools

import jax
import jax.numpy as jnp
from jax import lax
from jax.experimental import pallas as pl
from jax.experimental.pallas import tpu as pltpu
from jax.sharding import PartitionSpec as P

MESH = pl.DeviceIdType.MESH
LANES = 128


def chunk_list(width, tiles_each):
    bounds = list(range(0, width, tiles_each * LANES)) + [width]
    return list(zip(bounds[:-1], bounds[1:]))


def round_up(a, b):
    return (a + b - 1) // b * b


def gather_kernel(n_pp, n, m, chunks, x_hbm, g_hbm, u_hbm, h_hbm, w_hbm, g_out, x_out, passed_out, *scratch):
    (p_send, p_recv, pbuf, rbuf, xin, gin, uin, hin, wbuf, gbuf, xbuf, acc, in_sem, w_sem, out_sem, x_send, x_recv, xt_send, xt_recv,
     r_send, l_send, g_recv) = scratch
    p, d, t = lax.axis_index("pp"), lax.axis_index("dp"), lax.axis_index("tp")
    tokens, width = g_hbm.shape[2:]
    own_rows, feats = xbuf.shape[2:]
    padded = gbuf.shape[2]

    barrier = pltpu.get_barrier_semaphore()
    for i in range(1, n):
        pl.semaphore_signal(barrier, inc=1, device_id={"dp": lax.rem(d + i, n)}, device_id_type=MESH)
    for j in range(1, m):
        pl.semaphore_signal(barrier, inc=1, device_id={"tp": lax.rem(t + j, m)}, device_id_type=MESH)
    everyone = [(i, j) for j in range(m) for i in range(n)]

    def owner_of(stage, i, j):
        return {"pp": stage, "tp": lax.rem(t + j, m), "dp": lax.rem(d + i, n)}

    @pl.when(p > 0)
    def _():
        for i, j in everyone:
            pl.semaphore_signal(barrier, inc=1, device_id=owner_of(p - 1, i, j), device_id_type=MESH)

    @pl.when(p < n_pp - 1)
    def _():
        for i, j in everyone:
            pl.semaphore_signal(barrier, inc=1, device_id=owner_of(p + 1, i, j), device_id_type=MESH)


    loads = [
        pltpu.make_async_copy(src.at[0, 0], dst, in_sem.at[i])
        for i, (src, dst) in enumerate(((g_hbm, gin), (u_hbm, uin), (h_hbm, hin), (x_hbm, xin)))
    ]
    for load in loads:
        load.start()
    w_loads = []
    for c, (lo, hi) in enumerate(chunks):
        rows = pl.ds(lo, min(hi, width) - lo)
        whole = len(chunks) == 1
        source, target = (w_hbm.at[0], wbuf) if whole else (w_hbm.at[0, rows], wbuf.at[rows])
        w_loads.append(pltpu.make_async_copy(source, target, w_sem.at[c]))
        w_loads[c].start()
    acc[...] = jnp.zeros_like(acc)
    for load in loads[:3]:
        load.wait()
    if padded > width:
        last = padded - LANES
        gbuf[d, :, last:] = jnp.zeros((tokens, LANES), jnp.bfloat16)
    step_width = 4 * LANES
    for lo in range(0, width, step_width):
        hi = min(lo + step_width, width)
        gate = gin[:, lo:hi].astype(jnp.float32)
        up = uin[:, lo:hi].astype(jnp.float32)
        hidden = hin[:, lo:hi].astype(jnp.float32)
        sig = 1.0 / (1.0 + jnp.exp(-gate))
        gbuf[d, :, lo:hi] = (hidden * up * sig * (1.0 + gate * (1.0 - sig))).astype(jnp.bfloat16)
    loads[3].wait()
    sections = lax.div(p + n_pp - 1, n_pp) + lax.div(2 * n_pp - 2 - p, n_pp)
    pl.semaphore_wait(barrier, n - 1 + m - 1 + n * m * sections)

    x_copies = []
    for i in range(1, n):
        to = lax.rem(d + i, n)
        copy = pltpu.make_async_remote_copy(
            src_ref=xin.at[:, pl.ds(pl.multiple_of(to * feats, LANES), feats)],
            dst_ref=xbuf.at[t, d], send_sem=x_send.at[i], recv_sem=x_recv.at[d],
            device_id={"dp": to}, device_id_type=MESH)
        copy.start()
        x_copies.append(copy)
    x_local = pltpu.make_async_copy(
        xin.at[:, pl.ds(pl.multiple_of(d * feats, LANES), feats)], xbuf.at[t, d], out_sem.at[len(chunks)])
    x_local.start()

    def g_copy(block, c, to_right):
        lo, hi = chunks[c]
        cols = pl.ds(lo, min(hi, padded) - lo)
        sems = r_send if to_right else l_send
        return pltpu.make_async_remote_copy(
            src_ref=gbuf.at[block, :, cols], dst_ref=gbuf.at[block, :, cols],
            send_sem=sems.at[block, c], recv_sem=g_recv.at[block, c],
            device_id={"dp": d + 1 if to_right else d - 1}, device_id_type=MESH)

    x_tp = []
    for step in range(len(chunks) + n - 1):
        for k in range(n):
            c = step - k
            if c < 0 or c >= len(chunks):
                continue
            if k == 0:
                @pl.when(d < n - 1)
                def _():
                    g_copy(d, c, True).start()

                @pl.when(d > 0)
                def _():
                    g_copy(d, c, False).start()
            else:
                @pl.when(d - k >= 0)
                def _():
                    g_copy(d - k, c, True).wait_recv()

                    @pl.when(d < n - 1)
                    def _():
                        g_copy(d - k, c, True).start()

                @pl.when(d + k < n)
                def _():
                    g_copy(d + k, c, False).wait_recv()

                    @pl.when(d > 0)
                    def _():
                        g_copy(d + k, c, False).start()
        if step == 1:
            x_local.wait()
            for i in range(1, n):
                source = lax.rem(d + i, n)
                pltpu.make_async_remote_copy(
                    src_ref=xbuf.at[t, source], dst_ref=xbuf.at[t, source], send_sem=x_send.at[0],
                    recv_sem=x_recv.at[source], device_id={"dp": source}, device_id_type=MESH).wait_recv()
            for j in range(1, m):
                peer = lax.rem(t + j, m)
                copy = pltpu.make_async_remote_copy(
                    src_ref=xbuf.at[t], dst_ref=xbuf.at[t], send_sem=xt_send.at[j], recv_sem=xt_recv.at[t],
                    device_id={"tp": peer}, device_id_type=MESH)
                copy.start()
                x_tp.append(copy)
        if step == n - 1:
            for j in range(1, m):
                peer = lax.rem(t + j, m)
                pltpu.make_async_remote_copy(
                    src_ref=xbuf.at[peer], dst_ref=xbuf.at[peer], send_sem=xt_send.at[0],
                    recv_sem=xt_recv.at[peer], device_id={"tp": peer}, device_id_type=MESH).wait_recv()
            rows = [xbuf[j, r].astype(jnp.float32) for r in range(n) for j in range(m)]
            x_out[...] = jnp.concatenate(rows, axis=0).astype(jnp.bfloat16)
        done = step - (n - 1)
        if done >= 0:
            lo, hi = chunks[done]
            cols = pl.ds(lo, hi - lo)
            pltpu.make_async_copy(gbuf.at[:, :, cols], g_out.at[:, :, cols], out_sem.at[done]).start()
            hi = min(hi, width)
            w_loads[done].wait()
            grads = gbuf[:, :, lo:hi].reshape(n * tokens, hi - lo)
            acc[...] += lax.dot_general(
                grads, wbuf[lo:hi, :], (((1,), (0,)), ((), ())), preferred_element_type=jnp.float32)
    def pass_copy(i, j):
        return pltpu.make_async_remote_copy(
            src_ref=pbuf.at[j * n + i], dst_ref=rbuf.at[j * n + i],
            send_sem=p_send.at[j * n + i], recv_sem=p_recv.at[j * n + i],
            device_id=owner_of(p - 1, i, j), device_id_type=MESH)

    for i, j in everyone:
        start = lax.rem(d + i, n) * tokens + lax.rem(t + j, m) * own_rows
        rows = acc[pl.ds(pl.multiple_of(start, own_rows), own_rows), :]
        pbuf[j * n + i] = rows.astype(jnp.bfloat16)

    @pl.when(p > 0)
    def _():
        for i, j in everyone:
            pass_copy(i, j).start()

    for copy in x_copies + x_tp:
        copy.wait_send()
    for c, (lo, hi) in enumerate(chunks):
        cols = pl.ds(lo, hi - lo)
        pltpu.make_async_copy(gbuf.at[:, :, cols], g_out.at[:, :, cols], out_sem.at[c]).wait()
        for k in range(n):
            @pl.when((d - k >= 0) & (d < n - 1))
            def _():
                g_copy(d - k, c, True).wait_send()

            @pl.when((d + k < n) & (d > 0))
            def _():
                g_copy(d + k, c, False).wait_send()


    @pl.when(p < n_pp - 1)
    def _():
        for i, j in everyone:
            pass_copy(i, j).wait_recv()
        for i in range(n):
            total = rbuf[i].astype(jnp.float32)
            for j in range(1, m):
                total += rbuf[j * n + i].astype(jnp.float32)
            source = lax.rem(d - i + n, n)
            passed_out[:, pl.ds(pl.multiple_of(source * feats, LANES), feats)] = total.astype(jnp.bfloat16)

    @pl.when(p == n_pp - 1)
    def _():
        passed_out[...] = jnp.zeros_like(passed_out)

    @pl.when(p > 0)
    def _():
        for i, j in everyone:
            pass_copy(i, j).wait_send()


def weight_kernel(x_ref, g_ref, passed_ref, out_ref, passed_out):
    passed_out[...] = passed_ref[...]
    out_ref[...] = lax.dot_general(
        g_ref[...], x_ref[...], (((0,), (0,)), ((), ())), preferred_element_type=jnp.float32
    ).astype(out_ref.dtype)


def on_device(n_pp, n_tp, n_dp, layer_input, gate_pre, up_pre, hidden_grad, gate_weight):
    n, m = n_dp, n_tp
    tokens, width = gate_pre.shape[2:]
    own_rows, feats_all = layer_input.shape[2:]
    weights_t = jnp.swapaxes(gate_weight, 1, 2)
    feats = gate_weight.shape[1]
    padded = round_up(width, LANES)
    chunks = chunk_list(padded, 20)
    bf16, f32 = jnp.bfloat16, jnp.float32
    vmem, hbm = pltpu.VMEM, pl.BlockSpec(memory_space=pltpu.HBM)
    dma = pltpu.SemaphoreType.DMA
    results = pl.pallas_call(
        functools.partial(gather_kernel, n_pp, n, m, chunks),
        out_shape=[jax.ShapeDtypeStruct((n, tokens, padded), bf16), jax.ShapeDtypeStruct((n * tokens, feats), bf16)]
        + [jax.ShapeDtypeStruct((own_rows, feats_all), bf16)],
        in_specs=[hbm] * 5,
        out_specs=[pl.BlockSpec(memory_space=pl.ANY)] + [pl.BlockSpec(memory_space=vmem)] * 2,
        scratch_shapes=[
            dma((n * m,)), dma((n * m,)),
            vmem((n * m, own_rows, feats), bf16), vmem((n * m, own_rows, feats), bf16),
            vmem((own_rows, feats_all), bf16),
            vmem((tokens, width), bf16), vmem((tokens, width), bf16), vmem((tokens, width), bf16),
            vmem((width, feats), bf16),
            vmem((n, tokens, padded), bf16),
            vmem((m, n, own_rows, feats), bf16),
            vmem((n * tokens, feats), f32),
            dma((4,)), dma((len(chunks),)), dma((len(chunks) + 1,)),
            dma((n,)), dma((n,)), dma((m,)), dma((m,)),
            dma((n, len(chunks))), dma((n, len(chunks))), dma((n, len(chunks))),
        ],
        compiler_params=pltpu.CompilerParams(
            collective_id=0, has_side_effects=True, vmem_limit_bytes=58 * 1024 * 1024),
        cost_estimate=pl.CostEstimate(flops=2 * n * tokens * width * feats, bytes_accessed=16 * feats * width, transcendentals=0),
        name="gather",
    )(layer_input, gate_pre, up_pre, hidden_grad, weights_t)
    g_all, x_all, passed = results

    block = min(2048, padded)
    weight_out, passed = pl.pallas_call(
        weight_kernel,
        grid=(pl.cdiv(width, block),),
        out_shape=[jax.ShapeDtypeStruct((width, feats), bf16), jax.ShapeDtypeStruct((own_rows, feats_all), bf16)],
        in_specs=[
            pl.BlockSpec((n * tokens, feats), lambda i: (0, 0)),
            pl.BlockSpec((n * tokens, block), lambda i: (0, i)),
            pl.BlockSpec((own_rows, feats_all), lambda i: (0, 0)),
        ],
        out_specs=[pl.BlockSpec((block, feats), lambda i: (i, 0)), pl.BlockSpec((own_rows, feats_all), lambda i: (0, 0))],
        cost_estimate=pl.CostEstimate(flops=8 * n * tokens * width * feats, bytes_accessed=2 * feats * width, transcendentals=0),
        compiler_params=pltpu.CompilerParams(vmem_limit_bytes=58 * 1024 * 1024),
        name="weights",
    )(x_all, g_all.reshape(n * tokens, padded), passed)

    return passed[None, None], jnp.swapaxes(weight_out, 0, 1)[None]


def solution(mesh):
    return jax.shard_map(
        functools.partial(on_device, mesh.shape["pp"], mesh.shape["tp"], mesh.shape["dp"]),
        mesh=mesh,
        in_specs=(
            P("pp", "dp", "tp", None),
            P("pp", "dp", None, "tp"),
            P("pp", "dp", None, "tp"),
            P("pp", "dp", None, "tp"),
            P("pp", "dp", "tp"),
        ),
        out_specs=(P("pp", "dp", "tp", None), P("pp", "dp", "tp")),
        check_vma=False,
    )
```
